16 devices in a mesh: dp: 2 (over y, z), tp: 8 (over x, core).
Axes of the slice: x: 4, y: 2, z: 1, core: 2. Of those that a mesh axis runs over, the one named last changes fastest.
The devices are a block of a 4x4x8 slice.
Arguments:
- x: bfloat16 [4096, 7168], P('dp'), parts along dimension 0
- gain: bfloat16 [7168], replicated
- wq: bfloat16 [7168, 7168], P(None, 'tp')
- wk: bfloat16 [7168, 1024], P(None, 'tp')
- wv: bfloat16 [7168, 1024], P(None, 'tp')
- wo: bfloat16 [7168, 7168], P('tp')
Outputs:
- output: bfloat16 [4096, 7168], P('dp'), parts along dimension 0
There are 2 independent parts. The reference program is written for one: setup_inputs(seed, part) draws one part's arguments, and reference() takes and returns one part's arrays. A program takes and returns all parts, laid end to end along the dimension named above; an argument that names none is the same for every part.
All inputs are finite; a program needn't handle non-finite values.
Results may differ from the reference program's by a relative error of at most 0.012.
Values are sent between devices in bfloat16 or wider.
A program may use at most 768 MiB of HBM per device.

```python
import jax
import jax.numpy as jnp
from jax import lax

ROWS = 2048
D = 7168
HEADS = 56
KV_HEADS = 8
HEAD = 128
THETA = 10000


def setup_inputs(seed: int = 0, part: int = 0) -> dict:
    kx, kn, kq, kk, kv, ko = jax.random.split(jax.random.key(seed), 6)

    def weights(key, rows, columns):
        return jax.random.normal(key, (rows, columns), jnp.float32) * rows**-0.5

    drawn = {
        "x": jax.random.normal(jax.random.fold_in(kx, part), (ROWS, D), jnp.float32),
        "gain": 1 + 0.1 * jax.random.normal(kn, (D,), jnp.float32),
        "wq": 2 * weights(kq, D, HEADS * HEAD),
        "wk": 2 * weights(kk, D, KV_HEADS * HEAD),
        "wv": 4 * weights(kv, D, KV_HEADS * HEAD),
        "wo": weights(ko, HEADS * HEAD, D),
    }
    return {k: v.astype(jnp.bfloat16) for k, v in drawn.items()}


def normed(x, gain):
    wide = x.astype(jnp.float32)
    scale = lax.rsqrt(jnp.mean(wide * wide, -1, keepdims=True) + 1e-6)
    return (wide * scale * gain.astype(jnp.float32)).astype(jnp.bfloat16)


def turned(t, place, theta):
    half = t.shape[-1] // 2
    angle = place.astype(jnp.float32)[:, None] * theta ** (-jnp.arange(half, dtype=jnp.float32) / half)
    cos, sin = jnp.cos(angle)[:, None], jnp.sin(angle)[:, None]
    a, b = t[..., :half].astype(jnp.float32), t[..., half:].astype(jnp.float32)
    return jnp.concatenate([a * cos - b * sin, b * cos + a * sin], -1).astype(jnp.bfloat16)


def matmul(a, w):
    return jnp.dot(a, w, preferred_element_type=jnp.float32).astype(jnp.bfloat16)


def einsum(form, a, b):
    return jnp.einsum(form, a.astype(jnp.float32), b.astype(jnp.float32))


def attention(q, k, v):
    scores = einsum("tgsd,ugd->gstu", q, k) * q.shape[-1] ** -0.5
    token = jnp.arange(q.shape[0])
    scores = jnp.where(token[:, None] >= token, scores, -jnp.inf)
    weights = jax.nn.softmax(scores, -1).astype(jnp.bfloat16)
    return einsum("gstu,ugd->tgsd", weights, v).astype(jnp.bfloat16)


def reference(x, gain, wq, wk, wv, wo):
    a, place = normed(x, gain), jnp.arange(ROWS)
    q = turned(matmul(a, wq).reshape(ROWS, HEADS, HEAD), place, THETA).reshape(ROWS, KV_HEADS, -1, HEAD)
    k = turned(matmul(a, wk).reshape(ROWS, KV_HEADS, HEAD), place, THETA)
    v = matmul(a, wv).reshape(ROWS, KV_HEADS, HEAD)
    seen = attention(q, k, v).reshape(ROWS, HEADS * HEAD)
    return (x.astype(jnp.float32) + jnp.dot(seen, wo, preferred_element_type=jnp.float32)).astype(jnp.bfloat16)
```

```python
import functools

import jax
import jax.numpy as jnp
from jax import lax
from jax.experimental import pallas as pl
from jax.experimental.pallas import tpu as pltpu
from jax.sharding import PartitionSpec as P

HEAD = 128
THETA = 10000
NEG = -1e30
HIDDEN = 2 * NEG
LOG2E = 1.4426950408889634
CHUNK = 128
KEYS = 256
VMEM_LIMIT = 66_000_000
SLOTS = 4
LAG = 5
F32, BF16 = jnp.float32, jnp.bfloat16


def _dot(a, b, ca, cb):
    return lax.dot_general(a, b, (((ca,), (cb,)), ((), ())), preferred_element_type=F32)


def _strips(cols):
    if cols % 512 == 0 or cols <= 512:
        w = min(cols, 512)
        return [(at, w) for at in range(0, cols, w)]
    out, at = [], 0
    while at < cols:
        w = min(512, cols - at)
        out.append((at, w))
        at += w
    return out


def _kernel(x_hbm, gain_ref, off_ref, base_ref, wq_hbm, wk_hbm, wv_hbm, wo_hbm, y_hbm,
            w_s, wo_s, k_s, vt_s, x_s, a_s, q_s, seen_s, top_s, mix_s, gap_s,
            keep_s, dsend, drecv, r1send, r1recv, r2send, r2recv, xres, ysend,
            xsem, wsem, xrsem, d_s, d_r, r1s, r1r, r2s, r2r, g1s, g1r, lsem, g2s, g2r, fs, fr,
            *, chips, eps):
    rows, width = x_hbm.shape
    R = x_s.shape[1]
    C = rows // R
    R2 = R // 2
    RP = R2 // chips
    half = width // 2
    nq = wq_hbm.shape[1]
    heads = nq // HEAD
    cols = heads * R
    bk = gap_s.shape[0]
    e = HEAD**-0.5 * LOG2E

    me = lax.axis_index("tp")
    c = me // 2
    k = me % 2
    right = ((c + 1) % chips) * 2 + k
    left = ((c + chips - 1) % chips) * 2 + k
    sib = c * 2 + (1 - k)
    cr, cl, co = (c + 1) % chips, (c + chips - 1) % chips, (c + 2) % chips

    def to(dev):
        return dict(device_id={"tp": dev}, device_id_type=pl.DeviceIdType.MESH)

    def xload(t):
        return pltpu.make_async_copy(x_hbm.at[pl.ds(t * R, R), :], x_s.at[t % 2], xsem.at[t % 2])

    wloads = [
        pltpu.make_async_copy(wq_hbm, w_s.at[:, 0:nq], wsem.at[0]),
        pltpu.make_async_copy(wk_hbm, w_s.at[:, nq:nq + HEAD], wsem.at[1]),
        pltpu.make_async_copy(wv_hbm, w_s.at[:, nq + HEAD:nq + 2 * HEAD], wsem.at[2]),
    ]
    woload = pltpu.make_async_copy(wo_hbm, wo_s, wsem.at[3])
    xload(0).start()
    for w in wloads:
        w.start()
    woload.start()

    barrier = pltpu.get_barrier_semaphore()
    for dev in (right, left, sib):
        pl.semaphore_signal(barrier, inc=1, **to(dev))
    pl.semaphore_wait(barrier, 3)

    k_s[...] = jnp.zeros_like(k_s)
    vt_s[0:HEAD, :] = jnp.zeros((HEAD, rows), BF16)
    vt_s[HEAD:, :] = jnp.ones((vt_s.shape[0] - HEAD, rows), BF16)
    gap_s[...] = lax.rem(lax.broadcasted_iota(jnp.int32, (bk, cols), 1), R) - lax.broadcasted_iota(jnp.int32, (bk, cols), 0)

    def project(t):
        xload(t).wait()

        @pl.when(t + 1 < C)
        def _():
            xload(t + 1).start()

        slot = t % 2
        bw = width // 7

        def strip(r, _):
            here = pl.ds(pl.multiple_of(r * 16, 16), 16)
            acc = jnp.zeros((16, bw), F32)
            for b in range(7):
                w = x_s[slot, here, b * bw:(b + 1) * bw].astype(F32)
                acc = acc + w * w
            scale = lax.rsqrt(jnp.sum(acc, axis=-1, keepdims=True) * (1.0 / width) + eps)
            for b in range(7):
                w = x_s[slot, here, b * bw:(b + 1) * bw].astype(F32)
                a_s[here, b * bw:(b + 1) * bw] = (w * scale * gain_ref[0:1, b * bw:(b + 1) * bw].astype(F32)).astype(BF16)
            return 0

        lax.fori_loop(0, R // 16, strip, 0)

        @pl.when(t == 0)
        def _():
            for w in wloads:
                w.wait()

        cb, sb = base_ref[t, :, 0:HEAD], base_ref[t, :, HEAD:2 * HEAD]
        co_, so_ = off_ref[:, 0:HEAD], off_ref[:, HEAD:2 * HEAD]
        cos = cb * co_ - sb * so_
        sin = sb * co_ + cb * so_
        sin = jnp.where(lax.broadcasted_iota(jnp.int32, (R, HEAD), 1) < HEAD // 2, -sin, sin)

        def turn(z):
            z = z.astype(BF16).astype(F32)
            return (z * cos + pltpu.roll(z, HEAD // 2, 1) * sin).astype(BF16)

        got = _dot(a_s[...], w_s[...], 1, 0)
        for h in range(heads):
            q_s[h * R:(h + 1) * R, :] = turn(got[:, h * HEAD:(h + 1) * HEAD])
        here = pl.ds(pl.multiple_of(t * R, R), R)
        k_s[here, :] = turn(got[:, nq:nq + HEAD])
        vt_s[0:HEAD, here] = got[:, nq + HEAD:nq + 2 * HEAD].T.astype(BF16)

    def attend(t):
        top_s[...] = jnp.full(top_s.shape, NEG, F32)
        mix_s[...] = jnp.zeros(mix_s.shape, F32)
        strips = _strips(cols)

        def block(j, masked):
            here = pl.ds(pl.multiple_of(j * bk, bk), bk)
            scores = [_dot(k_s[here, :], q_s[at:at + w, :], 1, 1) for at, w in strips]
            weights, keeps = [], []
            for (at, w), s in zip(strips, scores):
                if masked:
                    s = jnp.where(gap_s[:, at:at + w] >= j * bk - t * R, s, HIDDEN)
                old = top_s[0:1, at:at + w]
                top = jnp.maximum(old, s.max(axis=0, keepdims=True))
                top_s[0:1, at:at + w] = top
                weights.append(jnp.exp2((s - top) * e).astype(BF16))
                keeps.append(jnp.exp2((old - top) * e))
            for (at, w), p, keep in zip(strips, weights, keeps):
                mix_s[:, at:at + w] = mix_s[:, at:at + w] * keep + _dot(vt_s[:, here], p, 1, 0)

        whole = (t * R) // bk
        last = (t * R + R + bk - 1) // bk
        lax.fori_loop(0, whole, lambda j, _: block(j, False), None)
        lax.fori_loop(whole, last, lambda j, _: block(j, True), None)
        low = pl.ds(pl.multiple_of(k * R2, R2), R2)
        high = pl.ds(pl.multiple_of((1 - k) * R2, R2), R2)
        for h in range(heads):
            at = slice(h * R, (h + 1) * R)
            out = (mix_s[0:HEAD, at] * (1 / mix_s[HEAD:HEAD + 1, at])).T.astype(BF16)
            seen_s[low, h * HEAD:(h + 1) * HEAD] = out[:R2]
            seen_s[high, h * HEAD:(h + 1) * HEAD] = out[R2:]

    def dcopy(t):
        return pltpu.make_async_remote_copy(dsend.at[t % 2], drecv.at[t % 2], d_s.at[t % 2], d_r.at[t % 2], **to(sib))

    def output(t):
        @pl.when(t == 0)
        def _():
            woload.wait()

        @pl.when(t >= 2)
        def _():
            dcopy(t - 2).wait_send()

        bn = width // 7

        def cols_of(b, _):
            at = pl.ds(pl.multiple_of(b * bn, bn), bn)
            o = _dot(seen_s[...], wo_s[:, at], 1, 0)
            keep_s[t % SLOTS, :, at] = o[:R2]
            dsend[t % 2, :, at] = o[R2:].astype(BF16)
            return 0

        lax.fori_loop(0, 7, cols_of, 0)
        dcopy(t).start()

    def part(p):
        return pl.ds(pl.multiple_of(p * RP, RP), RP)

    def place(j, p):
        return pl.ds(pl.multiple_of(j * R + k * R2 + p * RP, RP), RP)

    def r1copy(j, d):
        return pltpu.make_async_remote_copy(r1send.at[j % 2, d], r1recv.at[j % SLOTS, d], r1s.at[j % 2, d], r1r.at[j % SLOTS, d],
                                            **to(left if d else right))

    def r2copy(j, d):
        return pltpu.make_async_remote_copy(r2send.at[j % 2, d], r2recv.at[j % SLOTS, d], r2s.at[j % 2, d], r2r.at[j % SLOTS, d],
                                            **to(left if d else right))

    def xrload(j):
        return pltpu.make_async_copy(x_hbm.at[place(j, c), :], xres.at[j % 2], xrsem.at[j % 2])

    def g1copy(j, d):
        return pltpu.make_async_remote_copy(ysend.at[j % 2], y_hbm.at[place(j, c), :], g1s.at[j % 2, d], g1r.at[j % SLOTS, d],
                                            **to(left if d else right))

    def g1sib(j):
        return pltpu.make_async_remote_copy(ysend.at[j % 2], y_hbm.at[place(j, c), :], g1s.at[j % 2, 2], fr.at[0], **to(sib))

    def g1own(j):
        return pltpu.make_async_copy(ysend.at[j % 2], y_hbm.at[place(j, c), :], lsem.at[j % 2])

    def arrived1(j, d):
        ref = y_hbm.at[place(j, cr if d else cl), :]
        return pltpu.make_async_remote_copy(ref, ref, g1s.at[j % 2, d], g1r.at[j % SLOTS, d], **to(left if d else right))

    def g2copy(j, d):
        ref = y_hbm.at[place(j, cr if d else cl), (half if d else 0):(width if d else half)]
        return pltpu.make_async_remote_copy(ref, ref, g2s.at[0], g2r.at[j % SLOTS, d], **to(left if d else right))

    def arrived2(j, d):
        ref = y_hbm.at[place(j, co), (half if d else 0):(width if d else half)]
        return pltpu.make_async_remote_copy(ref, ref, g2s.at[0], g2r.at[j % SLOTS, d], **to(left if d else right))

    def forward(j, p):
        ref = y_hbm.at[place(j, p), :]
        return pltpu.make_async_remote_copy(ref, ref, fs.at[0], fr.at[0], **to(sib))

    def stage1(j):
        dcopy(j).wait_recv()

        @pl.when(j >= 2)
        def _():
            r1copy(j - 2, 0).wait_send()
            r1copy(j - 2, 1).wait_send()

        s4, s2 = j % SLOTS, j % 2
        v = keep_s[s4, part(co), :] + drecv[s2, part(co), :].astype(F32)
        r1send[s2, 0] = v[:, :half].astype(BF16)
        r1send[s2, 1] = v[:, half:].astype(BF16)
        for p in (cr, cl, c):
            keep_s[s4, part(p), :] = keep_s[s4, part(p), :] + drecv[s2, part(p), :].astype(F32)
        r1copy(j, 0).start()
        r1copy(j, 1).start()

    def stage2(j):
        r1copy(j, 0).wait_recv()
        r1copy(j, 1).wait_recv()

        @pl.when(j >= 2)
        def _():
            r2copy(j - 2, 0).wait_send()
            r2copy(j - 2, 1).wait_send()

        s4, s2 = j % SLOTS, j % 2
        r2send[s2, 0, :, :half] = (keep_s[s4, part(cr), :half] + r1recv[s4, 0].astype(F32)).astype(BF16)
        r2send[s2, 0, :, half:] = keep_s[s4, part(cr), half:].astype(BF16)
        r2send[s2, 1, :, :half] = keep_s[s4, part(cl), :half].astype(BF16)
        r2send[s2, 1, :, half:] = (keep_s[s4, part(cl), half:] + r1recv[s4, 1].astype(F32)).astype(BF16)
        xrload(j).start()
        r2copy(j, 0).start()
        r2copy(j, 1).start()

    def stage3(j):
        r2copy(j, 0).wait_recv()
        r2copy(j, 1).wait_recv()
        xrload(j).wait()

        @pl.when(j >= 2)
        def _():
            g1copy(j - 2, 0).wait_send()
            g1copy(j - 2, 1).wait_send()
            g1sib(j - 2).wait_send()
            g1own(j - 2).wait()

        s4, s2 = j % SLOTS, j % 2
        total = keep_s[s4, part(c), :] + r2recv[s4, 0].astype(F32) + r2recv[s4, 1].astype(F32)
        ysend[s2] = (xres[s2].astype(F32) + total).astype(BF16)
        g1copy(j, 0).start()
        g1copy(j, 1).start()
        g1sib(j).start()
        g1own(j).start()

    def stage4(j):
        arrived1(j, 0).wait_recv()
        g2copy(j, 0).start()
        arrived1(j, 1).wait_recv()
        g2copy(j, 1).start()
        forward(j, cl).start()
        forward(j, cr).start()

    def stage5(j):
        arrived2(j, 0).wait_recv()
        arrived2(j, 1).wait_recv()
        forward(j, co).start()

    def when(t, lag, f):
        @pl.when((t >= lag) & (t < C + lag))
        def _():
            f(t - lag)

    def step(t, _):
        when(t, 0, project)
        when(t, 1, stage1)
        when(t, 0, attend)
        when(t, 2, stage2)
        when(t, 3, stage3)
        when(t, 0, output)
        when(t, 4, stage4)
        when(t, 5, stage5)
        return 0

    lax.fori_loop(0, C + LAG, step, 0)

    for j in (C - 2, C - 1):
        dcopy(j).wait_send()
        for d in (0, 1):
            r1copy(j, d).wait_send()
            r2copy(j, d).wait_send()
            g1copy(j, d).wait_send()
        g1sib(j).wait_send()
        g1own(j).wait()
    all_sent2 = y_hbm.at[pl.ds(0, C * RP), :]
    pltpu.make_async_copy(all_sent2, all_sent2, g2s.at[0]).wait()
    sent = y_hbm.at[pl.ds(0, C * RP * (chips - 1)), :]
    pltpu.make_async_copy(sent, sent, fs.at[0]).wait()
    got = y_hbm.at[pl.ds(0, C * R2), :]
    pltpu.make_async_copy(got, got, fr.at[0]).wait()


def _fused(x, gain, off, base, wq, wk, wv, wo, chips):
    rows, width = x.shape
    nq = wq.shape[1]
    R = off.shape[0]
    R2, RP, half = R // 2, R // 2 // chips, width // 2
    cols = nq // HEAD * R
    any_, vmem = pl.BlockSpec(memory_space=pl.ANY), pl.BlockSpec(memory_space=pltpu.VMEM)
    dma = pltpu.SemaphoreType.DMA
    keys = nq // HEAD * HEAD * rows * rows
    return pl.pallas_call(
        functools.partial(_kernel, chips=chips, eps=1e-6),
        out_shape=jax.ShapeDtypeStruct((rows, width), BF16),
        in_specs=[any_, vmem, vmem, vmem, any_, any_, any_, any_],
        out_specs=any_,
        scratch_shapes=[
            pltpu.VMEM((width, nq + 2 * HEAD), BF16),
            pltpu.VMEM((nq, width), BF16),
            pltpu.VMEM((rows, HEAD), BF16),
            pltpu.VMEM((HEAD + 16, rows), BF16),
            pltpu.VMEM((2, R, width), BF16),
            pltpu.VMEM((R, width), BF16),
            pltpu.VMEM((cols, HEAD), BF16),
            pltpu.VMEM((R, nq), BF16),
            pltpu.VMEM((8, cols), F32),
            pltpu.VMEM((HEAD + 16, cols), F32),
            pltpu.VMEM((KEYS, cols), jnp.int32),
            pltpu.VMEM((SLOTS, R2, width), F32),
            pltpu.VMEM((2, R2, width), BF16),
            pltpu.VMEM((2, R2, width), BF16),
            pltpu.VMEM((2, 2, RP, half), BF16),
            pltpu.VMEM((SLOTS, 2, RP, half), BF16),
            pltpu.VMEM((2, 2, RP, width), BF16),
            pltpu.VMEM((SLOTS, 2, RP, width), BF16),
            pltpu.VMEM((2, RP, width), BF16),
            pltpu.VMEM((2, RP, width), BF16),
            dma((2,)), dma((4,)), dma((2,)),
            dma((2,)), dma((2,)),
            dma((2, 2)), dma((SLOTS, 2)),
            dma((2, 2)), dma((SLOTS, 2)),
            dma((2, 3)), dma((SLOTS, 2)), dma((2,)),
            dma((1,)), dma((SLOTS, 2)),
            dma((1,)), dma((1,)),
        ],
        compiler_params=pltpu.CompilerParams(collective_id=0, has_side_effects=True, vmem_limit_bytes=VMEM_LIMIT),
        cost_estimate=pl.CostEstimate(flops=2 * rows * width * (2 * nq + 2 * HEAD) + 2 * keys, transcendentals=keys // HEAD,
                                      bytes_accessed=2 * (4 * rows * width + 2 * width * nq)),
    )(x, gain, off, base, wq, wk, wv, wo)


def _angles(place):
    freq = THETA ** (-jnp.arange(HEAD // 2, dtype=F32) / (HEAD // 2))
    angle = place.astype(F32)[:, None] * freq
    cos, sin = jnp.cos(angle), jnp.sin(angle)
    return jnp.concatenate([cos, cos, sin, sin], -1)


def solution(mesh):
    chips = mesh.shape["tp"] // 2

    def step(x, gain, wq, wk, wv, wo):
        off = _angles(jnp.arange(CHUNK))
        base = _angles(jnp.arange(x.shape[0] // CHUNK) * CHUNK)
        return _fused(x, gain[None], off, base[:, None], wq, wk, wv, wo, chips)

    tokens, columns = P("dp", None), P(None, "tp")
    return jax.shard_map(
        step,
        mesh=mesh,
        in_specs=(tokens, P(None), columns, columns, columns, P("tp", None)),
        out_specs=tokens,
        check_vma=False,
    )
```

```python
import functools

import jax
import jax.numpy as jnp
from jax import lax
from jax.experimental import pallas as pl
from jax.experimental.pallas import tpu as pltpu
from jax.sharding import PartitionSpec as P

HEAD = 128
THETA = 10000
NEG = -1e30
HIDDEN = 2 * NEG
LOG2E = 1.4426950408889634
CHUNK = 128
KEYS = 256
VMEM_LIMIT = 36_000_000
SLOTS = 4
LAG = 4
SLICES = 4
F32, BF16 = jnp.float32, jnp.bfloat16


def _dot(a, b, ca, cb):
    return lax.dot_general(a, b, (((ca,), (cb,)), ((), ())), preferred_element_type=F32)


def _strips(cols):
    if cols % 512 == 0 or cols <= 512:
        w = min(cols, 512)
        return [(at, w) for at in range(0, cols, w)]
    out, at = [], 0
    while at < cols:
        w = min(512, cols - at)
        out.append((at, w))
        at += w
    return out


def _fit(size, want, unit=128):
    return max(n for n in range(unit, want + 1, unit) if size % n == 0)


def _kernel(x_hbm, gain_ref, angle_ref, wq_hbm, wk_hbm, wv_hbm, wo_hbm, y_hbm,
            w_s, wo_s, got_s, k_s, vt_s, x_s, a_s, q_s, seen_s, top_s, mix_s, gap_s,
            keep_s, dsend, drecv, r1send, r1recv, r2send, r2recv, xres, ysend,
            xsem, wsem, wosem, xrsem, d_s, d_r, r1s, r1r, r2s, r2r, g1s, g1r, lsem, g2s, g2r, fs, fr, psem,
            *, chips, eps):
    rows, width = x_hbm.shape
    R = x_s.shape[1]
    C = rows // R
    R2 = R // 2
    RP = R2 // chips
    half = width // 2
    nq = wq_hbm.shape[1]
    heads = nq // HEAD
    cols = heads * R
    bk = gap_s.shape[0]
    e = HEAD**-0.5 * LOG2E

    me = lax.axis_index("tp")
    c = me // 2
    k = me % 2
    right = ((c + 1) % chips) * 2 + k
    left = ((c + chips - 1) % chips) * 2 + k
    sib = c * 2 + (1 - k)
    cr, cl, co = (c + 1) % chips, (c + chips - 1) % chips, (c + 2) % chips

    def to(dev):
        return dict(device_id={"tp": dev}, device_id_type=pl.DeviceIdType.MESH)

    def xload(t):
        return pltpu.make_async_copy(x_hbm.at[pl.ds(t * R, R), :], x_s.at[t % 2], xsem.at[t % 2])

    ks = width // SLICES

    def wloads(n):
        at = slice(n * ks, (n + 1) * ks)
        return [
            pltpu.make_async_copy(wq_hbm.at[at, :], w_s.at[at, 0:nq], wsem.at[n, 0]),
            pltpu.make_async_copy(wk_hbm.at[at, :], w_s.at[at, nq:nq + HEAD], wsem.at[n, 1]),
            pltpu.make_async_copy(wv_hbm.at[at, :], w_s.at[at, nq + HEAD:nq + 2 * HEAD], wsem.at[n, 2]),
        ]

    woload = pltpu.make_async_copy(wo_hbm, wo_s, wosem.at[0])
    xload(0).start()
    for n in range(SLICES):
        for w in wloads(n):
            w.start()
    woload.start()

    barrier = pltpu.get_barrier_semaphore()
    for dev in (right, left, sib):
        pl.semaphore_signal(barrier, inc=1, **to(dev))
    pl.semaphore_wait(barrier, 3)

    k_s[...] = jnp.zeros_like(k_s)
    vt_s[0:HEAD, :] = jnp.zeros((HEAD, rows), BF16)
    vt_s[HEAD:, :] = jnp.ones((vt_s.shape[0] - HEAD, rows), BF16)
    gap_s[...] = lax.rem(lax.broadcasted_iota(jnp.int32, (bk, cols), 1), R) - lax.broadcasted_iota(jnp.int32, (bk, cols), 0)

    def project(t):
        xload(t).wait()

        @pl.when(t + 1 < C)
        def _():
            xload(t + 1).start()

        slot = t % 2
        bw = width // 7

        def strip(r, _):
            here = pl.ds(pl.multiple_of(r * 16, 16), 16)
            acc = jnp.zeros((16, bw), F32)
            for b in range(7):
                w = x_s[slot, here, b * bw:(b + 1) * bw].astype(F32)
                acc = acc + w * w
            scale = lax.rsqrt(jnp.sum(acc, axis=-1, keepdims=True) * (1.0 / width) + eps)
            for b in range(width // 128):
                at = slice(b * 128, (b + 1) * 128)
                a_s[here, at] = (x_s[slot, here, at].astype(F32) * scale * gain_ref[b:b + 1, :]).astype(BF16)
            return 0

        lax.fori_loop(0, R // 16, strip, 0)

        @pl.when(t == 0)
        def _():
            for n in range(SLICES):
                for w in wloads(n):
                    w.wait()
                at = slice(n * ks, (n + 1) * ks)
                term = _dot(a_s[:, at], w_s[at, :], 1, 0)
                got_s[...] = term if n == 0 else got_s[...] + term

        @pl.when(t > 0)
        def _():
            got_s[...] = _dot(a_s[...], w_s[...], 1, 0)

        chunks = angle_ref[R:R + C, :]
        base = jnp.sum(jnp.where(lax.broadcasted_iota(jnp.int32, chunks.shape, 0) == t, chunks, 0.0), axis=0, keepdims=True)
        cb, sb = base[:, 0:HEAD], base[:, HEAD:2 * HEAD]
        co_, so_ = angle_ref[0:R, 0:HEAD], angle_ref[0:R, HEAD:2 * HEAD]
        cos = cb * co_ - sb * so_
        sin = sb * co_ + cb * so_
        sin = jnp.where(lax.broadcasted_iota(jnp.int32, (R, HEAD), 1) < HEAD // 2, -sin, sin)

        def turn(z):
            z = z.astype(BF16).astype(F32)
            return (z * cos + pltpu.roll(z, HEAD // 2, 1) * sin).astype(BF16)

        for h in range(heads):
            q_s[h * R:(h + 1) * R, :] = turn(got_s[:, h * HEAD:(h + 1) * HEAD])
        here = pl.ds(pl.multiple_of(t * R, R), R)
        k_s[here, :] = turn(got_s[:, nq:nq + HEAD])
        vt_s[0:HEAD, here] = got_s[:, nq + HEAD:nq + 2 * HEAD].T.astype(BF16)

    def attend(t):
        top_s[...] = jnp.full(top_s.shape, NEG, F32)
        mix_s[...] = jnp.zeros(mix_s.shape, F32)
        strips = _strips(cols)

        def block(j, masked):
            here = pl.ds(pl.multiple_of(j * bk, bk), bk)
            scores = [_dot(k_s[here, :], q_s[at:at + w, :], 1, 1) for at, w in strips]
            weights, keeps = [], []
            for (at, w), s in zip(strips, scores):
                if masked:
                    s = jnp.where(gap_s[:, at:at + w] >= j * bk - t * R, s, HIDDEN)
                old = top_s[0:1, at:at + w]
                top = jnp.maximum(old, s.max(axis=0, keepdims=True))
                top_s[0:1, at:at + w] = top
                weights.append(jnp.exp2((s - top) * e).astype(BF16))
                keeps.append(jnp.exp2((old - top) * e))
            for (at, w), p, keep in zip(strips, weights, keeps):
                mix_s[:, at:at + w] = mix_s[:, at:at + w] * keep + _dot(vt_s[:, here], p, 1, 0)

        whole = (t * R) // bk
        last = (t * R + R + bk - 1) // bk
        lax.fori_loop(0, whole, lambda j, _: block(j, False), None)
        lax.fori_loop(whole, last, lambda j, _: block(j, True), None)
        low = pl.ds(pl.multiple_of(k * R2, R2), R2)
        high = pl.ds(pl.multiple_of((1 - k) * R2, R2), R2)
        for h in range(heads):
            at = slice(h * R, (h + 1) * R)
            out = (mix_s[0:HEAD, at] * (1 / mix_s[HEAD:HEAD + 1, at])).T.astype(BF16)
            seen_s[low, h * HEAD:(h + 1) * HEAD] = out[:R2]
            seen_s[high, h * HEAD:(h + 1) * HEAD] = out[R2:]

    def dcopy(t):
        return pltpu.make_async_remote_copy(dsend.at[t % 2], drecv.at[t % 2], d_s.at[t % 2], d_r.at[t % 2], **to(sib))

    def output(t):
        @pl.when(t == 0)
        def _():
            woload.wait()

        @pl.when(t >= 2)
        def _():
            dcopy(t - 2).wait_send()

        bn = width // 7

        for b in range(7):
            at = slice(b * bn, (b + 1) * bn)
            o = _dot(seen_s[...], wo_s[:, at], 1, 0)
            keep_s[t % SLOTS, :, at] = o[:R2]
            dsend[t % 2, :, at] = o[R2:].astype(BF16)
        dcopy(t).start()

    def part(p):
        return pl.ds(pl.multiple_of(p * RP, RP), RP)

    def place(j, p):
        return pl.ds(pl.multiple_of(j * R + k * R2 + p * RP, RP), RP)

    def r1copy(j, d):
        return pltpu.make_async_remote_copy(r1send.at[j % 2, d], r1recv.at[j % SLOTS, d], r1s.at[j % 2, d], r1r.at[j % SLOTS, d],
                                            **to(left if d else right))

    def r2copy(j, d):
        return pltpu.make_async_remote_copy(r2send.at[j % 2, d], r2recv.at[j % SLOTS, d], r2s.at[j % 2, d], r2r.at[j % SLOTS, d],
                                            **to(left if d else right))

    def xrload(j):
        return pltpu.make_async_copy(x_hbm.at[place(j, c), :], xres.at[j % 2], xrsem.at[j % 2])

    def g1copy(j, d):
        return pltpu.make_async_remote_copy(ysend.at[j % 2], y_hbm.at[place(j, c), :], g1s.at[j % 2, d], g1r.at[j % SLOTS, d],
                                            **to(left if d else right))

    def g1sib(j):
        return pltpu.make_async_remote_copy(ysend.at[j % 2], y_hbm.at[place(j, c), :], g1s.at[j % 2, 2], fr.at[j], **to(sib))

    def g1own(j):
        return pltpu.make_async_copy(ysend.at[j % 2], y_hbm.at[place(j, c), :], lsem.at[j % 2])

    def arrived1(j, d):
        ref = y_hbm.at[place(j, cr if d else cl), :]
        return pltpu.make_async_remote_copy(ref, ref, g1s.at[j % 2, d], g1r.at[j % SLOTS, d], **to(left if d else right))

    def g2copy(j, d):
        ref = y_hbm.at[place(j, cr if d else cl), (half if d else 0):(width if d else half)]
        return pltpu.make_async_remote_copy(ref, ref, g2s.at[0], g2r.at[j % SLOTS, d], **to(left if d else right))

    def arrived2(j, d):
        ref = y_hbm.at[place(j, co), (half if d else 0):(width if d else half)]
        return pltpu.make_async_remote_copy(ref, ref, g2s.at[0], g2r.at[j % SLOTS, d], **to(left if d else right))

    def forward(j, p):
        ref = y_hbm.at[place(j, p), :]
        return pltpu.make_async_remote_copy(ref, ref, fs.at[0], fr.at[j], **to(sib))

    def stage1(j):
        dcopy(j).wait_recv()

        @pl.when(j >= 2)
        def _():
            r1copy(j - 2, 0).wait_send()
            r1copy(j - 2, 1).wait_send()

        s4, s2 = j % SLOTS, j % 2
        v = keep_s[s4, part(co), :] + drecv[s2, part(co), :].astype(F32)
        r1send[s2, 0] = v[:, :half].astype(BF16)
        r1send[s2, 1] = v[:, half:].astype(BF16)
        for p in (cr, cl, c):
            keep_s[s4, part(p), :] = keep_s[s4, part(p), :] + drecv[s2, part(p), :].astype(F32)
        r1copy(j, 0).start()
        r1copy(j, 1).start()

    def stage2(j):
        r1copy(j, 0).wait_recv()
        r1copy(j, 1).wait_recv()

        @pl.when(j >= 2)
        def _():
            r2copy(j - 2, 0).wait_send()
            r2copy(j - 2, 1).wait_send()

        s4, s2 = j % SLOTS, j % 2
        r2send[s2, 0, :, :half] = (keep_s[s4, part(cr), :half] + r1recv[s4, 0].astype(F32)).astype(BF16)
        r2send[s2, 0, :, half:] = keep_s[s4, part(cr), half:].astype(BF16)
        r2send[s2, 1, :, :half] = keep_s[s4, part(cl), :half].astype(BF16)
        r2send[s2, 1, :, half:] = (keep_s[s4, part(cl), half:] + r1recv[s4, 1].astype(F32)).astype(BF16)
        xrload(j).start()
        r2copy(j, 0).start()
        r2copy(j, 1).start()

    def stage3(j):
        r2copy(j, 0).wait_recv()
        r2copy(j, 1).wait_recv()
        xrload(j).wait()

        @pl.when(j >= 2)
        def _():
            g1copy(j - 2, 0).wait_send()
            g1copy(j - 2, 1).wait_send()
            g1sib(j - 2).wait_send()
            g1own(j - 2).wait()

        s4, s2 = j % SLOTS, j % 2
        total = keep_s[s4, part(c), :] + r2recv[s4, 0].astype(F32) + r2recv[s4, 1].astype(F32)
        ysend[s2] = (xres[s2].astype(F32) + total).astype(BF16)
        g1copy(j, 0).start()
        g1copy(j, 1).start()
        g1sib(j).start()
        g1own(j).start()

    def stage4(j):
        arrived1(j, 0).wait_recv()
        g2copy(j, 0).start()
        arrived1(j, 1).wait_recv()
        g2copy(j, 1).start()
        forward(j, cl).start()
        forward(j, cr).start()

    def stage5(j):
        arrived2(j, 0).wait_recv()
        arrived2(j, 1).wait_recv()
        forward(j, co).start()

    bc = _fit(width, w_s.shape[1])
    first = bc // R
    last = first + nq // R

    def sibling_rows(j):
        ref = y_hbm.at[pl.ds(0, R2), :]
        return pltpu.make_async_copy(ref, ref, fr.at[j])

    def fill(j):
        here = pl.ds(pl.multiple_of((j - first) * R, R), R)
        return pltpu.make_async_copy(y_hbm.at[pl.ds(pl.multiple_of(j * R, R), R), :], wo_s.at[here, :], psem.at[1])

    def when(t, lag, f):
        @pl.when((t >= lag) & (t < C + lag))
        def _():
            f(t - lag)

    def step(t, _):
        when(t, 0, project)
        when(t, 1, stage1)
        when(t, 0, attend)
        when(t, 2, stage3)
        when(t, 3, stage4)
        when(t, 0, output)
        when(t, 1, stage2)
        when(t, 4, stage5)

        @pl.when(t == C)
        def _():
            for j in range(C - LAG):
                sibling_rows(j).wait()
            for b in range(width // bc):
                pltpu.make_async_copy(y_hbm.at[0:bc, b * bc:(b + 1) * bc], w_s.at[b * bc:(b + 1) * bc, 0:bc], psem.at[0]).start()
            for j in range(first, C - LAG):
                fill(j).start()

        @pl.when(t > C)
        def _():
            j = t - LAG - 1

            @pl.when(j == C - 2)
            def _():
                g1own(j).wait()

            sibling_rows(j).wait()
            fill(j).start()

        return 0

    lax.fori_loop(0, C + LAG, step, 0)

    for j in (C - 2, C - 1):
        dcopy(j).wait_send()
        for d in (0, 1):
            r1copy(j, d).wait_send()
            r2copy(j, d).wait_send()
            g1copy(j, d).wait_send()
        g1sib(j).wait_send()
    g1own(C - 1).wait()
    sibling_rows(C - 1).wait()
    for n, sem in ((C * RP, g2s.at[0]), (C * RP * (chips - 1), fs.at[0]), (first * R, psem.at[0]), ((last - first) * R, psem.at[1])):
        ref = y_hbm.at[pl.ds(0, n), :]
        pltpu.make_async_copy(ref, ref, sem).wait()


def _write(y_hbm, w_ref, wo_ref, out_hbm, rest, sem):
    rows, width = y_hbm.shape
    bc = _fit(width, w_ref.shape[1])
    done = bc + wo_ref.shape[0]
    load = pltpu.make_async_copy(y_hbm.at[done:rows, :], rest, sem.at[0])
    load.start()
    copies = [pltpu.make_async_copy(wo_ref, out_hbm.at[bc:done, :], sem.at[1])]
    for b in range(width // bc):
        copies.append(pltpu.make_async_copy(w_ref.at[b * bc:(b + 1) * bc, 0:bc], out_hbm.at[0:bc, b * bc:(b + 1) * bc], sem.at[2 + b]))
    for copy in copies:
        copy.start()
    load.wait()
    store = pltpu.make_async_copy(rest, out_hbm.at[done:rows, :], sem.at[0])
    store.start()
    for copy in copies:
        copy.wait()
    store.wait()


def _fused(x, gain, angles, wq, wk, wv, wo, chips):
    rows, width = x.shape
    nq = wq.shape[1]
    R = CHUNK
    R2, RP, half = R // 2, R // 2 // chips, width // 2
    cols = nq // HEAD * R
    any_, vmem = pl.BlockSpec(memory_space=pl.ANY), pl.BlockSpec(memory_space=pltpu.VMEM)
    dma = pltpu.SemaphoreType.DMA
    keys = nq // HEAD * HEAD * rows * rows
    y, w, o = pl.pallas_call(
        functools.partial(_kernel, chips=chips, eps=1e-6),
        out_shape=[jax.ShapeDtypeStruct((rows, width), BF16), pltpu.VMEM((width, nq + 2 * HEAD), BF16), pltpu.VMEM((nq, width), BF16)],
        in_specs=[any_, vmem, vmem, any_, any_, any_, any_],
        out_specs=[any_, vmem, vmem],
        scratch_shapes=[
            pltpu.VMEM((R, nq + 2 * HEAD), F32),
            pltpu.VMEM((rows, HEAD), BF16),
            pltpu.VMEM((HEAD + 16, rows), BF16),
            pltpu.VMEM((2, R, width), BF16),
            pltpu.VMEM((R, width), BF16),
            pltpu.VMEM((cols, HEAD), BF16),
            pltpu.VMEM((R, nq), BF16),
            pltpu.VMEM((8, cols), F32),
            pltpu.VMEM((HEAD + 16, cols), F32),
            pltpu.VMEM((KEYS, cols), jnp.int32),
            pltpu.VMEM((SLOTS, R2, width), F32),
            pltpu.VMEM((2, R2, width), BF16),
            pltpu.VMEM((2, R2, width), BF16),
            pltpu.VMEM((2, 2, RP, half), BF16),
            pltpu.VMEM((SLOTS, 2, RP, half), BF16),
            pltpu.VMEM((2, 2, RP, width), BF16),
            pltpu.VMEM((SLOTS, 2, RP, width), BF16),
            pltpu.VMEM((2, RP, width), BF16),
            pltpu.VMEM((2, RP, width), BF16),
            dma((2,)), dma((SLICES, 3)), dma((1,)), dma((2,)),
            dma((2,)), dma((2,)),
            dma((2, 2)), dma((SLOTS, 2)),
            dma((2, 2)), dma((SLOTS, 2)),
            dma((2, 3)), dma((SLOTS, 2)), dma((2,)),
            dma((1,)), dma((SLOTS, 2)),
            dma((1,)), dma((rows // R,)), dma((2,)),
        ],
        compiler_params=pltpu.CompilerParams(collective_id=0, has_side_effects=True, vmem_limit_bytes=VMEM_LIMIT),
        cost_estimate=pl.CostEstimate(flops=2 * rows * width * (2 * nq + 2 * HEAD) + 2 * keys, transcendentals=keys // HEAD,
                                      bytes_accessed=2 * (4 * rows * width + 2 * width * nq)),
    )(x, gain, angles, wq, wk, wv, wo)
    bc = _fit(width, nq + 2 * HEAD)
    return pl.pallas_call(
        _write,
        out_shape=jax.ShapeDtypeStruct((rows, width), BF16),
        in_specs=[any_, vmem, vmem],
        out_specs=any_,
        scratch_shapes=[pltpu.VMEM((rows - bc - nq, width), BF16), dma((2 + width // bc,))],
        compiler_params=pltpu.CompilerParams(vmem_limit_bytes=2_500_000),
        cost_estimate=pl.CostEstimate(flops=0, transcendentals=0, bytes_accessed=4 * rows * width),
    )(y, w, o)


def _angles(place):
    freq = THETA ** (-jnp.arange(HEAD // 2, dtype=F32) / (HEAD // 2))
    angle = place.astype(F32)[:, None] * freq
    cos, sin = jnp.cos(angle), jnp.sin(angle)
    return jnp.concatenate([cos, cos, sin, sin], -1)


def solution(mesh):
    chips = mesh.shape["tp"] // 2

    def step(x, gain, wq, wk, wv, wo):
        place = jnp.arange(CHUNK + x.shape[0] // CHUNK)
        angles = _angles(jnp.where(place < CHUNK, place, (place - CHUNK) * CHUNK))
        return _fused(x, gain.astype(F32).reshape(-1, 128), angles, wq, wk, wv, wo, chips)

    tokens, columns = P("dp", None), P(None, "tp")
    return jax.shard_map(
        step,
        mesh=mesh,
        in_specs=(tokens, P(None), columns, columns, columns, P("tp", None)),
        out_specs=tokens,
        check_vma=False,
    )
```

```python
import functools

import jax
import jax.numpy as jnp
import numpy as np
from jax import lax
from jax.experimental import pallas as pl
from jax.experimental.pallas import tpu as pltpu
from jax.sharding import PartitionSpec as P

HEAD = 128
THETA = 10000
NEG = -1e30
HIDDEN = 2 * NEG
LOG2E = 1.4426950408889634
CHUNK = 128
KEYS = 256
VMEM_LIMIT = 36_000_000
SLOTS = 4
LAG = 4
SLICES = 7
AHEAD = 5
F32, BF16 = jnp.float32, jnp.bfloat16


def _dot(a, b, ca, cb):
    return lax.dot_general(a, b, (((ca,), (cb,)), ((), ())), preferred_element_type=F32)


def _strips(cols):
    if cols % 512 == 0 or cols <= 512:
        w = min(cols, 512)
        return [(at, w) for at in range(0, cols, w)]
    out, at = [], 0
    while at < cols:
        w = min(512, cols - at)
        out.append((at, w))
        at += w
    return out


def _fit(size, want, unit=128):
    return max(n for n in range(unit, want + 1, unit) if size % n == 0)


def _kernel(x_hbm, gain_hbm, angle_hbm, wq_hbm, wk_hbm, wv_hbm, wo_hbm, y_hbm,
            w_s, wo_s, gain_s, gain_ref, angle_ref, got_s, k_s, vt_s, x_s, a_s, q_s, seen_s, top_s, mix_s, gap_s,
            keep_s, dsend, drecv, r1send, r1recv, r2send, r2recv, xres, ysend,
            xsem, wsem, wosem, xrsem, d_s, d_r, r1s, r1r, r2s, r2r, g1s, g1r, lsem, g2s, g2r, fs, fr, psem, csem,
            *, chips, eps):
    rows, width = x_hbm.shape
    R = x_s.shape[1]
    C = rows // R
    R2 = R // 2
    RP = R2 // chips
    half = width // 2
    nq = wq_hbm.shape[1]
    heads = nq // HEAD
    cols = heads * R
    bk = gap_s.shape[0]
    e = HEAD**-0.5 * LOG2E

    me = lax.axis_index("tp")
    c = me // 2
    k = me % 2
    right = ((c + 1) % chips) * 2 + k
    left = ((c + chips - 1) % chips) * 2 + k
    sib = c * 2 + (1 - k)
    cr, cl, co = (c + 1) % chips, (c + chips - 1) % chips, (c + 2) % chips

    def to(dev):
        return dict(device_id={"tp": dev}, device_id_type=pl.DeviceIdType.MESH)

    def xload(t):
        return pltpu.make_async_copy(x_hbm.at[pl.ds(t * R, R), :], x_s.at[t % 2], xsem.at[t % 2])

    ks = width // SLICES

    def wloads(n):
        at = slice(n * ks, (n + 1) * ks)
        return [
            pltpu.make_async_copy(wq_hbm.at[at, :], w_s.at[at, 0:nq], wsem.at[n, 0]),
            pltpu.make_async_copy(wk_hbm.at[at, :], w_s.at[at, nq:nq + HEAD], wsem.at[n, 1]),
            pltpu.make_async_copy(wv_hbm.at[at, :], w_s.at[at, nq + HEAD:nq + 2 * HEAD], wsem.at[n, 2]),
        ]

    bn = width // 7

    def woload(b):
        at = slice(b * bn, (b + 1) * bn)
        return pltpu.make_async_copy(wo_hbm.at[:, at], wo_s.at[:, at], wosem.at[b])

    small = [pltpu.make_async_copy(gain_hbm, gain_s, csem.at[0]), pltpu.make_async_copy(angle_hbm, angle_ref, csem.at[1])]
    xload(0).start()
    for copy in small:
        copy.start()

    def fetch(n):
        if n < SLICES:
            for w in wloads(n):
                w.start()
        elif n < SLICES + 7:
            woload(n - SLICES).start()

    for n in range(AHEAD):
        fetch(n)

    barrier = pltpu.get_barrier_semaphore()
    for dev in (right, left, sib):
        pl.semaphore_signal(barrier, inc=1, **to(dev))

    k_s[...] = jnp.zeros_like(k_s)
    vt_s[0:HEAD, :] = jnp.zeros((HEAD, rows), BF16)
    vt_s[HEAD:, :] = jnp.ones((vt_s.shape[0] - HEAD, rows), BF16)
    gap_s[...] = lax.rem(lax.broadcasted_iota(jnp.int32, (bk, cols), 1), R) - lax.broadcasted_iota(jnp.int32, (bk, cols), 0)

    for copy in small:
        copy.wait()
    for b in range(width // 128):
        gain_ref[0:1, b * 128:(b + 1) * 128] = gain_s[b * 128:(b + 1) * 128].astype(F32)[None, :]

    def normed(t):
        xload(t).wait()

        @pl.when((t > 0) & (t + 1 < C))
        def _():
            xload(t + 1).start()

        slot = t % 2
        bw = width // 7

        def strip(r, _):
            here = pl.ds(pl.multiple_of(r * 16, 16), 16)
            acc = jnp.zeros((16, bw), F32)
            for b in range(7):
                w = x_s[slot, here, b * bw:(b + 1) * bw].astype(F32)
                acc = acc + w * w
            scale = lax.rsqrt(jnp.sum(acc, axis=-1, keepdims=True) * (1.0 / width) + eps)
            for b in range(width // 128):
                at = slice(b * 128, (b + 1) * 128)
                a_s[here, at] = (x_s[slot, here, at].astype(F32) * scale * gain_ref[0:1, at]).astype(BF16)
            return 0

        lax.fori_loop(0, R // 16, strip, 0)

    normed(0)
    pl.semaphore_wait(barrier, 3)

    def project(t):
        @pl.when(t == 0)
        def _():
            for n in range(SLICES):
                for w in wloads(n):
                    w.wait()
                fetch(n + AHEAD)
                at = slice(n * ks, (n + 1) * ks)
                term = _dot(a_s[:, at], w_s[at, :], 1, 0)
                got_s[...] = term if n == 0 else got_s[...] + term

        @pl.when(t > 0)
        def _():
            got_s[...] = _dot(a_s[...], w_s[...], 1, 0)

        chunks = angle_ref[R:R + C, :]
        base = jnp.sum(jnp.where(lax.broadcasted_iota(jnp.int32, chunks.shape, 0) == t, chunks, 0.0), axis=0, keepdims=True)
        cb, sb = base[:, 0:HEAD], base[:, HEAD:2 * HEAD]
        co_, so_ = angle_ref[0:R, 0:HEAD], angle_ref[0:R, HEAD:2 * HEAD]
        cos = cb * co_ - sb * so_
        sin = sb * co_ + cb * so_
        sin = jnp.where(lax.broadcasted_iota(jnp.int32, (R, HEAD), 1) < HEAD // 2, -sin, sin)

        def turn(z):
            z = z.astype(BF16).astype(F32)
            return (z * cos + pltpu.roll(z, HEAD // 2, 1) * sin).astype(BF16)

        for h in range(heads):
            q_s[h * R:(h + 1) * R, :] = turn(got_s[:, h * HEAD:(h + 1) * HEAD])
        here = pl.ds(pl.multiple_of(t * R, R), R)
        k_s[here, :] = turn(got_s[:, nq:nq + HEAD])
        vt_s[0:HEAD, here] = got_s[:, nq + HEAD:nq + 2 * HEAD].T.astype(BF16)

    def attend(t):
        top_s[...] = jnp.full(top_s.shape, NEG, F32)
        mix_s[...] = jnp.zeros(mix_s.shape, F32)
        strips = _strips(cols)

        def block(j, masked):
            here = pl.ds(pl.multiple_of(j * bk, bk), bk)
            scores = [_dot(k_s[here, :], q_s[at:at + w, :], 1, 1) for at, w in strips]
            weights, keeps = [], []
            for (at, w), s in zip(strips, scores):
                if masked:
                    s = jnp.where(gap_s[:, at:at + w] >= j * bk - t * R, s, HIDDEN)
                old = top_s[0:1, at:at + w]
                top = jnp.maximum(old, s.max(axis=0, keepdims=True))
                top_s[0:1, at:at + w] = top
                weights.append(jnp.exp2((s - top) * e).astype(BF16))
                keeps.append(jnp.exp2((old - top) * e))
            for (at, w), p, keep in zip(strips, weights, keeps):
                mix_s[:, at:at + w] = mix_s[:, at:at + w] * keep + _dot(vt_s[:, here], p, 1, 0)

        whole = (t * R) // bk
        last = (t * R + R + bk - 1) // bk
        lax.fori_loop(0, whole, lambda j, _: block(j, False), None)
        lax.fori_loop(whole, last, lambda j, _: block(j, True), None)
        low = pl.ds(pl.multiple_of(k * R2, R2), R2)
        high = pl.ds(pl.multiple_of((1 - k) * R2, R2), R2)
        for h in range(heads):
            at = slice(h * R, (h + 1) * R)
            out = (mix_s[0:HEAD, at] * (1 / mix_s[HEAD:HEAD + 1, at])).T.astype(BF16)
            seen_s[low, h * HEAD:(h + 1) * HEAD] = out[:R2]
            seen_s[high, h * HEAD:(h + 1) * HEAD] = out[R2:]

    def dcopy(t):
        return pltpu.make_async_remote_copy(dsend.at[t % 2], drecv.at[t % 2], d_s.at[t % 2], d_r.at[t % 2], **to(sib))

    def output(t):
        @pl.when(t >= 2)
        def _():
            dcopy(t - 2).wait_send()

        def columns(b):
            at = slice(b * bn, (b + 1) * bn)
            o = _dot(seen_s[...], wo_s[:, at], 1, 0)
            keep_s[t % SLOTS, :, at] = o[:R2]
            dsend[t % 2, :, at] = o[R2:].astype(BF16)

        @pl.when(t == 0)
        def _():
            for b in range(7):
                woload(b).wait()
                fetch(SLICES + b + AHEAD)
                if b == 7 - AHEAD:
                    xload(1).start()
                columns(b)

        @pl.when(t > 0)
        def _():
            for b in range(7):
                columns(b)

        dcopy(t).start()

    def part(p):
        return pl.ds(pl.multiple_of(p * RP, RP), RP)

    def place(j, p):
        return pl.ds(pl.multiple_of(j * R + k * R2 + p * RP, RP), RP)

    def r1copy(j, d):
        return pltpu.make_async_remote_copy(r1send.at[j % 2, d], r1recv.at[j % SLOTS, d], r1s.at[j % 2, d], r1r.at[j % SLOTS, d],
                                            **to(left if d else right))

    def r2copy(j, d, h):
        at = slice(half, width) if h else slice(0, half)
        return pltpu.make_async_remote_copy(r2send.at[j % 2, d, :, at], r2recv.at[j % SLOTS, d, :, at], r2s.at[j % 2, d, h],
                                            r2r.at[j % SLOTS, d, h], **to(left if d else right))

    def xrload(j):
        return pltpu.make_async_copy(x_hbm.at[place(j, c), :], xres.at[j % 2], xrsem.at[j % 2])

    def g1copy(j, d):
        return pltpu.make_async_remote_copy(ysend.at[j % 2], y_hbm.at[place(j, c), :], g1s.at[j % 2, d], g1r.at[j % SLOTS, d],
                                            **to(left if d else right))

    def g1sib(j):
        return pltpu.make_async_remote_copy(ysend.at[j % 2], y_hbm.at[place(j, c), :], g1s.at[j % 2, 2], fr.at[j], **to(sib))

    def g1own(j):
        return pltpu.make_async_copy(ysend.at[j % 2], y_hbm.at[place(j, c), :], lsem.at[j % 2])

    def arrived1(j, d):
        ref = y_hbm.at[place(j, cr if d else cl), :]
        return pltpu.make_async_remote_copy(ref, ref, g1s.at[j % 2, d], g1r.at[j % SLOTS, d], **to(left if d else right))

    def g2copy(j, d):
        ref = y_hbm.at[place(j, cr if d else cl), (half if d else 0):(width if d else half)]
        return pltpu.make_async_remote_copy(ref, ref, g2s.at[0], g2r.at[j % SLOTS, d], **to(left if d else right))

    def arrived2(j, d):
        ref = y_hbm.at[place(j, co), (half if d else 0):(width if d else half)]
        return pltpu.make_async_remote_copy(ref, ref, g2s.at[0], g2r.at[j % SLOTS, d], **to(left if d else right))

    def forward(j, p):
        ref = y_hbm.at[place(j, p), :]
        return pltpu.make_async_remote_copy(ref, ref, fs.at[0], fr.at[j], **to(sib))

    def stage1(j):
        dcopy(j).wait_recv()

        @pl.when(j >= 2)
        def _():
            r1copy(j - 2, 0).wait_send()
            r1copy(j - 2, 1).wait_send()
            r2copy(j - 2, 0, 1).wait_send()
            r2copy(j - 2, 1, 0).wait_send()

        s4, s2 = j % SLOTS, j % 2
        v = keep_s[s4, part(co), :] + drecv[s2, part(co), :].astype(F32)
        r1send[s2, 0] = v[:, :half].astype(BF16)
        r1send[s2, 1] = v[:, half:].astype(BF16)
        r1copy(j, 0).start()
        r1copy(j, 1).start()
        for p, d, ours, theirs in ((cr, 0, slice(half, width), slice(0, half)), (cl, 1, slice(0, half), slice(half, width))):
            r2send[s2, d, :, ours] = (keep_s[s4, part(p), ours] + drecv[s2, part(p), ours].astype(F32)).astype(BF16)
            keep_s[s4, part(p), theirs] = keep_s[s4, part(p), theirs] + drecv[s2, part(p), theirs].astype(F32)
        keep_s[s4, part(c), :] = keep_s[s4, part(c), :] + drecv[s2, part(c), :].astype(F32)
        r2copy(j, 0, 1).start()
        r2copy(j, 1, 0).start()

    def stage2(j):
        r1copy(j, 0).wait_recv()
        r1copy(j, 1).wait_recv()

        @pl.when(j >= 2)
        def _():
            r2copy(j - 2, 0, 0).wait_send()
            r2copy(j - 2, 1, 1).wait_send()

        s4, s2 = j % SLOTS, j % 2
        r2send[s2, 0, :, :half] = (keep_s[s4, part(cr), :half] + r1recv[s4, 0].astype(F32)).astype(BF16)
        r2send[s2, 1, :, half:] = (keep_s[s4, part(cl), half:] + r1recv[s4, 1].astype(F32)).astype(BF16)
        r2copy(j, 0, 0).start()
        r2copy(j, 1, 1).start()
        xrload(j).start()

    def stage3(j):
        for d in (0, 1):
            r2copy(j, d, 0).wait_recv()
            r2copy(j, d, 1).wait_recv()
        xrload(j).wait()

        @pl.when(j >= 2)
        def _():
            g1copy(j - 2, 0).wait_send()
            g1copy(j - 2, 1).wait_send()
            g1sib(j - 2).wait_send()
            g1own(j - 2).wait()

        s4, s2 = j % SLOTS, j % 2
        total = keep_s[s4, part(c), :] + r2recv[s4, 0].astype(F32) + r2recv[s4, 1].astype(F32)
        ysend[s2] = (xres[s2].astype(F32) + total).astype(BF16)
        g1copy(j, 0).start()
        g1copy(j, 1).start()
        g1sib(j).start()
        g1own(j).start()

    def stage4(j):
        arrived1(j, 0).wait_recv()
        g2copy(j, 0).start()
        arrived1(j, 1).wait_recv()
        g2copy(j, 1).start()
        forward(j, cl).start()
        forward(j, cr).start()

    def stage5(j):
        arrived2(j, 0).wait_recv()
        arrived2(j, 1).wait_recv()
        forward(j, co).start()

    bc = _fit(width, w_s.shape[1])
    first = bc // R
    last = first + nq // R

    def sibling_rows(j):
        ref = y_hbm.at[pl.ds(0, R2), :]
        return pltpu.make_async_copy(ref, ref, fr.at[j])

    def fill(j):
        here = pl.ds(pl.multiple_of((j - first) * R, R), R)
        return pltpu.make_async_copy(y_hbm.at[pl.ds(pl.multiple_of(j * R, R), R), :], wo_s.at[here, :], psem.at[1])

    def when(t, lag, f):
        @pl.when((t >= lag) & (t < C + lag))
        def _():
            f(t - lag)

    def step(t, _):
        @pl.when((t > 0) & (t < C))
        def _():
            normed(t)

        when(t, 1, stage1)
        when(t, 0, project)
        when(t, 0, attend)
        when(t, 2, stage3)
        when(t, 0, output)
        when(t, 1, stage2)
        when(t, 3, stage4)
        when(t, 4, stage5)

        @pl.when(t == C)
        def _():
            for j in range(C - LAG):
                sibling_rows(j).wait()
            for b in range(width // bc):
                pltpu.make_async_copy(y_hbm.at[0:bc, b * bc:(b + 1) * bc], w_s.at[b * bc:(b + 1) * bc, 0:bc], psem.at[0]).start()
            for j in range(first, C - LAG):
                fill(j).start()

        @pl.when(t > C)
        def _():
            j = t - LAG - 1

            @pl.when(j == C - 2)
            def _():
                g1own(j).wait()

            sibling_rows(j).wait()
            fill(j).start()

        return 0

    lax.fori_loop(0, C + LAG, step, 0)

    for j in (C - 2, C - 1):
        dcopy(j).wait_send()
        for d in (0, 1):
            r1copy(j, d).wait_send()
            r2copy(j, d, 0).wait_send()
            r2copy(j, d, 1).wait_send()
            g1copy(j, d).wait_send()
        g1sib(j).wait_send()
    g1own(C - 1).wait()
    sibling_rows(C - 1).wait()
    for n, sem in ((C * RP, g2s.at[0]), (C * RP * (chips - 1), fs.at[0]), (first * R, psem.at[0]), ((last - first) * R, psem.at[1])):
        ref = y_hbm.at[pl.ds(0, n), :]
        pltpu.make_async_copy(ref, ref, sem).wait()


def _write(y_hbm, w_ref, wo_ref, out_hbm, rest, sem):
    rows, width = y_hbm.shape
    bc = _fit(width, w_ref.shape[1])
    done = bc + wo_ref.shape[0]
    load = pltpu.make_async_copy(y_hbm.at[done:rows, :], rest, sem.at[0])
    load.start()
    copies = [pltpu.make_async_copy(wo_ref, out_hbm.at[bc:done, :], sem.at[1])]
    for b in range(width // bc):
        copies.append(pltpu.make_async_copy(w_ref.at[b * bc:(b + 1) * bc, 0:bc], out_hbm.at[0:bc, b * bc:(b + 1) * bc], sem.at[2 + b]))
    for copy in copies:
        copy.start()
    load.wait()
    store = pltpu.make_async_copy(rest, out_hbm.at[done:rows, :], sem.at[0])
    store.start()
    for copy in copies:
        copy.wait()
    store.wait()


def _fused(x, gain, angles, wq, wk, wv, wo, chips):
    rows, width = x.shape
    nq = wq.shape[1]
    R = CHUNK
    R2, RP, half = R // 2, R // 2 // chips, width // 2
    cols = nq // HEAD * R
    any_, vmem = pl.BlockSpec(memory_space=pl.ANY), pl.BlockSpec(memory_space=pltpu.VMEM)
    dma = pltpu.SemaphoreType.DMA
    keys = nq // HEAD * HEAD * rows * rows
    y, w, o = pl.pallas_call(
        functools.partial(_kernel, chips=chips, eps=1e-6),
        out_shape=[jax.ShapeDtypeStruct((rows, width), BF16), pltpu.VMEM((width, nq + 2 * HEAD), BF16), pltpu.VMEM((nq, width), BF16)],
        in_specs=[any_] * 7,
        out_specs=[any_, vmem, vmem],
        scratch_shapes=[
            pltpu.VMEM((width,), BF16),
            pltpu.VMEM((1, width), F32),
            pltpu.VMEM(angles.shape, F32),
            pltpu.VMEM((R, nq + 2 * HEAD), F32),
            pltpu.VMEM((rows, HEAD), BF16),
            pltpu.VMEM((HEAD + 16, rows), BF16),
            pltpu.VMEM((2, R, width), BF16),
            pltpu.VMEM((R, width), BF16),
            pltpu.VMEM((cols, HEAD), BF16),
            pltpu.VMEM((R, nq), BF16),
            pltpu.VMEM((8, cols), F32),
            pltpu.VMEM((HEAD + 16, cols), F32),
            pltpu.VMEM((KEYS, cols), jnp.int32),
            pltpu.VMEM((SLOTS, R2, width), F32),
            pltpu.VMEM((2, R2, width), BF16),
            pltpu.VMEM((2, R2, width), BF16),
            pltpu.VMEM((2, 2, RP, half), BF16),
            pltpu.VMEM((SLOTS, 2, RP, half), BF16),
            pltpu.VMEM((2, 2, RP, width), BF16),
            pltpu.VMEM((SLOTS, 2, RP, width), BF16),
            pltpu.VMEM((2, RP, width), BF16),
            pltpu.VMEM((2, RP, width), BF16),
            dma((2,)), dma((SLICES, 3)), dma((7,)), dma((2,)),
            dma((2,)), dma((2,)),
            dma((2, 2)), dma((SLOTS, 2)),
            dma((2, 2, 2)), dma((SLOTS, 2, 2)),
            dma((2, 3)), dma((SLOTS, 2)), dma((2,)),
            dma((1,)), dma((SLOTS, 2)),
            dma((1,)), dma((rows // R,)), dma((2,)), dma((2,)),
        ],
        compiler_params=pltpu.CompilerParams(collective_id=0, has_side_effects=True, vmem_limit_bytes=VMEM_LIMIT),
        cost_estimate=pl.CostEstimate(flops=2 * rows * width * (2 * nq + 2 * HEAD) + 2 * keys, transcendentals=keys // HEAD,
                                      bytes_accessed=2 * (4 * rows * width + 2 * width * nq)),
    )(x, gain, angles, wq, wk, wv, wo)
    bc = _fit(width, nq + 2 * HEAD)
    return pl.pallas_call(
        _write,
        out_shape=jax.ShapeDtypeStruct((rows, width), BF16),
        in_specs=[any_, vmem, vmem],
        out_specs=any_,
        scratch_shapes=[pltpu.VMEM((rows - bc - nq, width), BF16), dma((2 + width // bc,))],
        compiler_params=pltpu.CompilerParams(vmem_limit_bytes=2_500_000),
        cost_estimate=pl.CostEstimate(flops=0, transcendentals=0, bytes_accessed=4 * rows * width),
    )(y, w, o)


def _angles(chunks):
    place = np.concatenate([np.arange(CHUNK), np.arange(chunks) * CHUNK]).astype(np.float32)
    freq = np.float32(THETA) ** (-np.arange(HEAD // 2, dtype=np.float32) / np.float32(HEAD // 2))
    angle = place[:, None] * freq
    cos, sin = np.cos(angle), np.sin(angle)
    return np.concatenate([cos, cos, sin, sin], -1)


def solution(mesh):
    chips = mesh.shape["tp"] // 2

    def step(x, gain, wq, wk, wv, wo):
        angles = jnp.asarray(_angles(x.shape[0] // CHUNK))
        return _fused(x, gain, angles, wq, wk, wv, wo, chips)

    tokens, columns = P("dp", None), P(None, "tp")
    return jax.shard_map(
        step,
        mesh=mesh,
        in_specs=(tokens, P(None), columns, columns, columns, P("tp", None)),
        out_specs=tokens,
        check_vma=False,
    )
```

```python
import functools

import jax
import jax.numpy as jnp
import numpy as np
from jax import lax
from jax.experimental import pallas as pl
from jax.experimental.pallas import tpu as pltpu
from jax.sharding import PartitionSpec as P

HEAD = 128
THETA = 10000
NEG = -1e30
HIDDEN = 2 * NEG
LOG2E = 1.4426950408889634
CHUNK = 128
KEYS = 256
VMEM_LIMIT = 36_000_000
SLOTS = 4
LAG = 4
SLICES = 7
AHEAD = 5
F32, BF16 = jnp.float32, jnp.bfloat16


def _dot(a, b, ca, cb):
    return lax.dot_general(a, b, (((ca,), (cb,)), ((), ())), preferred_element_type=F32)


def _strips(cols):
    if cols % 512 == 0 or cols <= 512:
        w = min(cols, 512)
        return [(at, w) for at in range(0, cols, w)]
    out, at = [], 0
    while at < cols:
        w = min(512, cols - at)
        out.append((at, w))
        at += w
    return out


def _fit(size, want, unit=128):
    return max(n for n in range(unit, want + 1, unit) if size % n == 0)


def _kernel(x_hbm, gain_hbm, angle_hbm, wq_hbm, wk_hbm, wv_hbm, wo_hbm, y_hbm,
            w_s, wo_s, gain_s, gain_ref, angle_ref, got_s, k_s, vt_s, x_s, a_s, q_s, seen_s, top_s, mix_s, gap_s,
            keep_s, dsend, drecv, r1send, r1recv, r2send, r2recv, xres, ysend,
            xsem, wsem, wosem, xrsem, d_s, d_r, r1s, r1r, r2s, r2r, g1s, g1r, lsem, g2s, g2r, fs, fr, psem, csem,
            *, chips, eps):
    rows, width = x_hbm.shape
    R = x_s.shape[1]
    C = rows // R
    R2 = R // 2
    RP = R2 // chips
    half = width // 2
    nq = wq_hbm.shape[1]
    heads = nq // HEAD
    cols = heads * R
    bk = gap_s.shape[0]
    e = HEAD**-0.5 * LOG2E

    me = lax.axis_index("tp")
    c = me // 2
    k = me % 2
    right = ((c + 1) % chips) * 2 + k
    left = ((c + chips - 1) % chips) * 2 + k
    sib = c * 2 + (1 - k)
    cr, cl, co = (c + 1) % chips, (c + chips - 1) % chips, (c + 2) % chips

    def to(dev):
        return dict(device_id={"tp": dev}, device_id_type=pl.DeviceIdType.MESH)

    def xload(t):
        return pltpu.make_async_copy(x_hbm.at[pl.ds(t * R, R), :], x_s.at[t % 2], xsem.at[t % 2])

    ks = width // SLICES

    def wloads(n):
        at = slice(n * ks, (n + 1) * ks)
        return [
            pltpu.make_async_copy(wq_hbm.at[at, :], w_s.at[at, 0:nq], wsem.at[n, 0]),
            pltpu.make_async_copy(wk_hbm.at[at, :], w_s.at[at, nq:nq + HEAD], wsem.at[n, 1]),
            pltpu.make_async_copy(wv_hbm.at[at, :], w_s.at[at, nq + HEAD:nq + 2 * HEAD], wsem.at[n, 2]),
        ]

    bn = width // 7

    def woload(b):
        at = slice(b * bn, (b + 1) * bn)
        return pltpu.make_async_copy(wo_hbm.at[:, at], wo_s.at[:, at], wosem.at[b])

    small = [pltpu.make_async_copy(gain_hbm, gain_s, csem.at[0]), pltpu.make_async_copy(angle_hbm, angle_ref, csem.at[1])]
    xload(0).start()
    for copy in small:
        copy.start()

    def fetch(n):
        if n < SLICES:
            for w in wloads(n):
                w.start()
        elif n < SLICES + 7:
            woload(n - SLICES).start()

    for n in range(AHEAD):
        fetch(n)

    barrier = pltpu.get_barrier_semaphore()
    for dev in (right, left, sib):
        pl.semaphore_signal(barrier, inc=1, **to(dev))

    k_s[...] = jnp.zeros_like(k_s)
    vt_s[0:HEAD, :] = jnp.zeros((HEAD, rows), BF16)
    vt_s[HEAD:, :] = jnp.ones((vt_s.shape[0] - HEAD, rows), BF16)
    gap_s[...] = lax.rem(lax.broadcasted_iota(jnp.int32, (bk, cols), 1), R) - lax.broadcasted_iota(jnp.int32, (bk, cols), 0)

    for copy in small:
        copy.wait()
    for b in range(width // 128):
        gain_ref[0:1, b * 128:(b + 1) * 128] = gain_s[b * 128:(b + 1) * 128].astype(F32)[None, :]

    def normed(t):
        xload(t).wait()

        @pl.when((t > 0) & (t + 1 < C))
        def _():
            xload(t + 1).start()

        slot = t % 2
        bw = width // 7

        def strip(r, _):
            here = pl.ds(pl.multiple_of(r * 16, 16), 16)
            acc = jnp.zeros((16, bw), F32)
            for b in range(7):
                w = x_s[slot, here, b * bw:(b + 1) * bw].astype(F32)
                acc = acc + w * w
            scale = lax.rsqrt(jnp.sum(acc, axis=-1, keepdims=True) * (1.0 / width) + eps)
            for b in range(width // 128):
                at = slice(b * 128, (b + 1) * 128)
                a_s[here, at] = (x_s[slot, here, at].astype(F32) * scale * gain_ref[0:1, at]).astype(BF16)
            return 0

        lax.fori_loop(0, R // 16, strip, 0)

    normed(0)
    pl.semaphore_wait(barrier, 3)

    def project(t):
        @pl.when(t == 0)
        def _():
            for n in range(SLICES):
                for w in wloads(n):
                    w.wait()
                fetch(n + AHEAD)
                at = slice(n * ks, (n + 1) * ks)
                term = _dot(a_s[:, at], w_s[at, :], 1, 0)
                got_s[...] = term if n == 0 else got_s[...] + term

        @pl.when(t > 0)
        def _():
            got_s[...] = _dot(a_s[...], w_s[...], 1, 0)

        chunks = angle_ref[R:R + C, :]
        base = jnp.sum(jnp.where(lax.broadcasted_iota(jnp.int32, chunks.shape, 0) == t, chunks, 0.0), axis=0, keepdims=True)
        cb, sb = base[:, 0:HEAD], base[:, HEAD:2 * HEAD]
        co_, so_ = angle_ref[0:R, 0:HEAD], angle_ref[0:R, HEAD:2 * HEAD]
        cos = cb * co_ - sb * so_
        sin = sb * co_ + cb * so_
        sin = jnp.where(lax.broadcasted_iota(jnp.int32, (R, HEAD), 1) < HEAD // 2, -sin, sin)

        def turn(z):
            z = z.astype(BF16).astype(F32)
            return (z * cos + pltpu.roll(z, HEAD // 2, 1) * sin).astype(BF16)

        for h in range(heads):
            q_s[h * R:(h + 1) * R, :] = turn(got_s[:, h * HEAD:(h + 1) * HEAD])
        here = pl.ds(pl.multiple_of(t * R, R), R)
        k_s[here, :] = turn(got_s[:, nq:nq + HEAD])
        vt_s[0:HEAD, here] = got_s[:, nq + HEAD:nq + 2 * HEAD].T.astype(BF16)

    def attend(t):
        top_s[...] = jnp.full(top_s.shape, NEG, F32)
        mix_s[...] = jnp.zeros(mix_s.shape, F32)
        strips = _strips(cols)

        def block(j, masked):
            here = pl.ds(pl.multiple_of(j * bk, bk), bk)
            scores = [_dot(k_s[here, :], q_s[at:at + w, :], 1, 1) for at, w in strips]
            weights, keeps = [], []
            for (at, w), s in zip(strips, scores):
                if masked:
                    s = jnp.where(gap_s[:, at:at + w] >= j * bk - t * R, s, HIDDEN)
                old = top_s[0:1, at:at + w]
                top = jnp.maximum(old, s.max(axis=0, keepdims=True))
                top_s[0:1, at:at + w] = top
                weights.append(jnp.exp2((s - top) * e).astype(BF16))
                keeps.append(jnp.exp2((old - top) * e))
            for (at, w), p, keep in zip(strips, weights, keeps):
                mix_s[:, at:at + w] = mix_s[:, at:at + w] * keep + _dot(vt_s[:, here], p, 1, 0)

        whole = (t * R) // bk
        last = (t * R + R + bk - 1) // bk
        lax.fori_loop(0, whole, lambda j, _: block(j, False), None)
        lax.fori_loop(whole, last, lambda j, _: block(j, True), None)
        low = pl.ds(pl.multiple_of(k * R2, R2), R2)
        high = pl.ds(pl.multiple_of((1 - k) * R2, R2), R2)
        for h in range(heads):
            at = slice(h * R, (h + 1) * R)
            out = (mix_s[0:HEAD, at] * (1 / mix_s[HEAD:HEAD + 1, at])).T.astype(BF16)
            seen_s[low, h * HEAD:(h + 1) * HEAD] = out[:R2]
            seen_s[high, h * HEAD:(h + 1) * HEAD] = out[R2:]

    cut = 4 * bn

    def dcopy(t, h):
        at = slice(cut, width) if h else slice(0, cut)
        return pltpu.make_async_remote_copy(dsend.at[t % 2, :, at], drecv.at[t % 2, :, at], d_s.at[t % 2, h], d_r.at[t % 2, h], **to(sib))

    def output(t):
        @pl.when(t >= 2)
        def _():
            dcopy(t - 2, 0).wait_send()
            dcopy(t - 2, 1).wait_send()

        def columns(b):
            at = slice(b * bn, (b + 1) * bn)
            o = _dot(seen_s[...], wo_s[:, at], 1, 0)
            keep_s[t % SLOTS, :, at] = o[:R2]
            dsend[t % 2, :, at] = o[R2:].astype(BF16)
            if (b + 1) * bn == cut:
                dcopy(t, 0).start()

        @pl.when(t == 0)
        def _():
            for b in range(7):
                woload(b).wait()
                fetch(SLICES + b + AHEAD)
                if b == 7 - AHEAD:
                    xload(1).start()
                columns(b)

        @pl.when(t > 0)
        def _():
            for b in range(7):
                columns(b)

        dcopy(t, 1).start()

    def part(p):
        return pl.ds(pl.multiple_of(p * RP, RP), RP)

    def place(j, p):
        return pl.ds(pl.multiple_of(j * R + k * R2 + p * RP, RP), RP)

    def r1copy(j, d):
        return pltpu.make_async_remote_copy(r1send.at[j % 2, d], r1recv.at[j % SLOTS, d], r1s.at[j % 2, d], r1r.at[j % SLOTS, d],
                                            **to(left if d else right))

    def r2copy(j, d, h):
        at = slice(half, width) if h else slice(0, half)
        return pltpu.make_async_remote_copy(r2send.at[j % 2, d, :, at], r2recv.at[j % SLOTS, d, :, at], r2s.at[j % 2, d, h],
                                            r2r.at[j % SLOTS, d, h], **to(left if d else right))

    def xrload(j):
        return pltpu.make_async_copy(x_hbm.at[place(j, c), :], xres.at[j % 2], xrsem.at[j % 2])

    def g1copy(j, d):
        return pltpu.make_async_remote_copy(ysend.at[j % 2], y_hbm.at[place(j, c), :], g1s.at[j % 2, d], g1r.at[j % SLOTS, d],
                                            **to(left if d else right))

    def g1sib(j):
        return pltpu.make_async_remote_copy(ysend.at[j % 2], y_hbm.at[place(j, c), :], g1s.at[j % 2, 2], fr.at[j], **to(sib))

    def g1own(j):
        return pltpu.make_async_copy(ysend.at[j % 2], y_hbm.at[place(j, c), :], lsem.at[j % 2])

    def arrived1(j, d):
        ref = y_hbm.at[place(j, cr if d else cl), :]
        return pltpu.make_async_remote_copy(ref, ref, g1s.at[j % 2, d], g1r.at[j % SLOTS, d], **to(left if d else right))

    def g2copy(j, d):
        ref = y_hbm.at[place(j, cr if d else cl), (half if d else 0):(width if d else half)]
        return pltpu.make_async_remote_copy(ref, ref, g2s.at[0], g2r.at[j % SLOTS, d], **to(left if d else right))

    def arrived2(j, d):
        ref = y_hbm.at[place(j, co), (half if d else 0):(width if d else half)]
        return pltpu.make_async_remote_copy(ref, ref, g2s.at[0], g2r.at[j % SLOTS, d], **to(left if d else right))

    def forward(j, p):
        ref = y_hbm.at[place(j, p), :]
        return pltpu.make_async_remote_copy(ref, ref, fs.at[0], fr.at[j], **to(sib))

    def stage1(j):
        dcopy(j, 0).wait_recv()
        dcopy(j, 1).wait_recv()

        @pl.when(j >= 2)
        def _():
            r1copy(j - 2, 0).wait_send()
            r1copy(j - 2, 1).wait_send()
            r2copy(j - 2, 0, 1).wait_send()
            r2copy(j - 2, 1, 0).wait_send()

        s4, s2 = j % SLOTS, j % 2
        v = keep_s[s4, part(co), :] + drecv[s2, part(co), :].astype(F32)
        r1send[s2, 0] = v[:, :half].astype(BF16)
        r1send[s2, 1] = v[:, half:].astype(BF16)
        r1copy(j, 0).start()
        r1copy(j, 1).start()
        for p, d, ours, theirs in ((cr, 0, slice(half, width), slice(0, half)), (cl, 1, slice(0, half), slice(half, width))):
            r2send[s2, d, :, ours] = (keep_s[s4, part(p), ours] + drecv[s2, part(p), ours].astype(F32)).astype(BF16)
            keep_s[s4, part(p), theirs] = keep_s[s4, part(p), theirs] + drecv[s2, part(p), theirs].astype(F32)
        keep_s[s4, part(c), :] = keep_s[s4, part(c), :] + drecv[s2, part(c), :].astype(F32)
        r2copy(j, 0, 1).start()
        r2copy(j, 1, 0).start()

    def stage2(j):
        r1copy(j, 0).wait_recv()
        r1copy(j, 1).wait_recv()

        @pl.when(j >= 2)
        def _():
            r2copy(j - 2, 0, 0).wait_send()
            r2copy(j - 2, 1, 1).wait_send()

        s4, s2 = j % SLOTS, j % 2
        r2send[s2, 0, :, :half] = (keep_s[s4, part(cr), :half] + r1recv[s4, 0].astype(F32)).astype(BF16)
        r2send[s2, 1, :, half:] = (keep_s[s4, part(cl), half:] + r1recv[s4, 1].astype(F32)).astype(BF16)
        r2copy(j, 0, 0).start()
        r2copy(j, 1, 1).start()
        xrload(j).start()

    def stage3(j):
        for d in (0, 1):
            r2copy(j, d, 0).wait_recv()
            r2copy(j, d, 1).wait_recv()
        xrload(j).wait()

        @pl.when(j >= 2)
        def _():
            g1copy(j - 2, 0).wait_send()
            g1copy(j - 2, 1).wait_send()
            g1sib(j - 2).wait_send()
            g1own(j - 2).wait()

        s4, s2 = j % SLOTS, j % 2
        total = keep_s[s4, part(c), :] + r2recv[s4, 0].astype(F32) + r2recv[s4, 1].astype(F32)
        ysend[s2] = (xres[s2].astype(F32) + total).astype(BF16)
        g1copy(j, 0).start()
        g1copy(j, 1).start()
        g1sib(j).start()
        g1own(j).start()

    def stage4(j):
        arrived1(j, 0).wait_recv()
        g2copy(j, 0).start()
        arrived1(j, 1).wait_recv()
        g2copy(j, 1).start()
        forward(j, cl).start()
        forward(j, cr).start()

    def stage5(j):
        arrived2(j, 0).wait_recv()
        arrived2(j, 1).wait_recv()
        forward(j, co).start()

    bc = _fit(width, w_s.shape[1])
    first = bc // R
    last = first + nq // R

    def sibling_rows(j):
        ref = y_hbm.at[pl.ds(0, R2), :]
        return pltpu.make_async_copy(ref, ref, fr.at[j])

    def fill(j):
        here = pl.ds(pl.multiple_of((j - first) * R, R), R)
        return pltpu.make_async_copy(y_hbm.at[pl.ds(pl.multiple_of(j * R, R), R), :], wo_s.at[here, :], psem.at[1])

    def when(t, lag, f):
        @pl.when((t >= lag) & (t < C + lag))
        def _():
            f(t - lag)

    def step(t, _):
        @pl.when((t > 0) & (t < C))
        def _():
            normed(t)

        when(t, 1, stage1)
        when(t, 0, project)
        when(t, 0, attend)
        when(t, 2, stage3)
        when(t, 0, output)
        when(t, 1, stage2)
        when(t, 3, stage4)
        when(t, 4, stage5)

        @pl.when(t == C)
        def _():
            for j in range(C - LAG):
                sibling_rows(j).wait()
            for b in range(width // bc):
                pltpu.make_async_copy(y_hbm.at[0:bc, b * bc:(b + 1) * bc], w_s.at[b * bc:(b + 1) * bc, 0:bc], psem.at[0]).start()
            for j in range(first, C - LAG):
                fill(j).start()

        @pl.when(t > C)
        def _():
            j = t - LAG - 1

            @pl.when(j == C - 2)
            def _():
                g1own(j).wait()

            sibling_rows(j).wait()
            fill(j).start()

        return 0

    lax.fori_loop(0, C + LAG, step, 0)

    for j in (C - 2, C - 1):
        dcopy(j, 0).wait_send()
        dcopy(j, 1).wait_send()
        for d in (0, 1):
            r1copy(j, d).wait_send()
            r2copy(j, d, 0).wait_send()
            r2copy(j, d, 1).wait_send()
            g1copy(j, d).wait_send()
        g1sib(j).wait_send()
    g1own(C - 1).wait()
    sibling_rows(C - 1).wait()
    for n, sem in ((C * RP, g2s.at[0]), (C * RP * (chips - 1), fs.at[0]), (first * R, psem.at[0]), ((last - first) * R, psem.at[1])):
        ref = y_hbm.at[pl.ds(0, n), :]
        pltpu.make_async_copy(ref, ref, sem).wait()


def _write(y_hbm, w_ref, wo_ref, out_hbm, rest, sem):
    rows, width = y_hbm.shape
    bc = _fit(width, w_ref.shape[1])
    done = bc + wo_ref.shape[0]
    load = pltpu.make_async_copy(y_hbm.at[done:rows, :], rest, sem.at[0])
    load.start()
    copies = [pltpu.make_async_copy(wo_ref, out_hbm.at[bc:done, :], sem.at[1])]
    for b in range(width // bc):
        copies.append(pltpu.make_async_copy(w_ref.at[b * bc:(b + 1) * bc, 0:bc], out_hbm.at[0:bc, b * bc:(b + 1) * bc], sem.at[2 + b]))
    for copy in copies:
        copy.start()
    load.wait()
    store = pltpu.make_async_copy(rest, out_hbm.at[done:rows, :], sem.at[0])
    store.start()
    for copy in copies:
        copy.wait()
    store.wait()


def _fused(x, gain, angles, wq, wk, wv, wo, chips):
    rows, width = x.shape
    nq = wq.shape[1]
    R = CHUNK
    R2, RP, half = R // 2, R // 2 // chips, width // 2
    cols = nq // HEAD * R
    any_, vmem = pl.BlockSpec(memory_space=pl.ANY), pl.BlockSpec(memory_space=pltpu.VMEM)
    dma = pltpu.SemaphoreType.DMA
    keys = nq // HEAD * HEAD * rows * rows
    y, w, o = pl.pallas_call(
        functools.partial(_kernel, chips=chips, eps=1e-6),
        out_shape=[jax.ShapeDtypeStruct((rows, width), BF16), pltpu.VMEM((width, nq + 2 * HEAD), BF16), pltpu.VMEM((nq, width), BF16)],
        in_specs=[any_] * 7,
        out_specs=[any_, vmem, vmem],
        scratch_shapes=[
            pltpu.VMEM((width,), BF16),
            pltpu.VMEM((1, width), F32),
            pltpu.VMEM(angles.shape, F32),
            pltpu.VMEM((R, nq + 2 * HEAD), F32),
            pltpu.VMEM((rows, HEAD), BF16),
            pltpu.VMEM((HEAD + 16, rows), BF16),
            pltpu.VMEM((2, R, width), BF16),
            pltpu.VMEM((R, width), BF16),
            pltpu.VMEM((cols, HEAD), BF16),
            pltpu.VMEM((R, nq), BF16),
            pltpu.VMEM((8, cols), F32),
            pltpu.VMEM((HEAD + 16, cols), F32),
            pltpu.VMEM((KEYS, cols), jnp.int32),
            pltpu.VMEM((SLOTS, R2, width), F32),
            pltpu.VMEM((2, R2, width), BF16),
            pltpu.VMEM((2, R2, width), BF16),
            pltpu.VMEM((2, 2, RP, half), BF16),
            pltpu.VMEM((SLOTS, 2, RP, half), BF16),
            pltpu.VMEM((2, 2, RP, width), BF16),
            pltpu.VMEM((SLOTS, 2, RP, width), BF16),
            pltpu.VMEM((2, RP, width), BF16),
            pltpu.VMEM((2, RP, width), BF16),
            dma((2,)), dma((SLICES, 3)), dma((7,)), dma((2,)),
            dma((2, 2)), dma((2, 2)),
            dma((2, 2)), dma((SLOTS, 2)),
            dma((2, 2, 2)), dma((SLOTS, 2, 2)),
            dma((2, 3)), dma((SLOTS, 2)), dma((2,)),
            dma((1,)), dma((SLOTS, 2)),
            dma((1,)), dma((rows // R,)), dma((2,)), dma((2,)),
        ],
        compiler_params=pltpu.CompilerParams(collective_id=0, has_side_effects=True, vmem_limit_bytes=VMEM_LIMIT),
        cost_estimate=pl.CostEstimate(flops=2 * rows * width * (2 * nq + 2 * HEAD) + 2 * keys, transcendentals=keys // HEAD,
                                      bytes_accessed=2 * (4 * rows * width + 2 * width * nq)),
    )(x, gain, angles, wq, wk, wv, wo)
    bc = _fit(width, nq + 2 * HEAD)
    return pl.pallas_call(
        _write,
        out_shape=jax.ShapeDtypeStruct((rows, width), BF16),
        in_specs=[any_, vmem, vmem],
        out_specs=any_,
        scratch_shapes=[pltpu.VMEM((rows - bc - nq, width), BF16), dma((2 + width // bc,))],
        compiler_params=pltpu.CompilerParams(vmem_limit_bytes=2_500_000),
        cost_estimate=pl.CostEstimate(flops=0, transcendentals=0, bytes_accessed=4 * rows * width),
    )(y, w, o)


def _angles(chunks):
    place = np.concatenate([np.arange(CHUNK), np.arange(chunks) * CHUNK]).astype(np.float32)
    freq = np.float32(THETA) ** (-np.arange(HEAD // 2, dtype=np.float32) / np.float32(HEAD // 2))
    angle = place[:, None] * freq
    cos, sin = np.cos(angle), np.sin(angle)
    return np.concatenate([cos, cos, sin, sin], -1)


def solution(mesh):
    chips = mesh.shape["tp"] // 2

    def step(x, gain, wq, wk, wv, wo):
        angles = jnp.asarray(_angles(x.shape[0] // CHUNK))
        return _fused(x, gain, angles, wq, wk, wv, wo, chips)

    tokens, columns = P("dp", None), P(None, "tp")
    return jax.shard_map(
        step,
        mesh=mesh,
        in_specs=(tokens, P(None), columns, columns, columns, P("tp", None)),
        out_specs=tokens,
        check_vma=False,
    )
```
